128 devices in a mesh: ctx: 16 (over y_hi, x, core), head: 8 (over y_lo, z).
Axes of the slice: x: 4, y: 4 (y_hi: 2, y_lo: 2; y = y_hi * 2 + y_lo), z: 4, core: 2. Of those that a mesh axis runs over, the one named last changes fastest.
Arguments:
- tokens: bfloat16 [2048, 8192], P('ctx', 'head'), may hold values from -6 to 6
- norm_gain: float32 [8192], replicated, may hold values from 0.1 to 1.9
- query_weight: bfloat16 [8192, 8192], P(None, 'head'), may hold values from -0.0625 to 0.0625
- key_weight: bfloat16 [8192, 1024], P(None, 'head'), may hold values from -0.0625 to 0.0625
- value_weight: bfloat16 [8192, 1024], P(None, 'head'), may hold values from -0.0625 to 0.0625
- cache_keys: bfloat16 [16384, 1024], P('ctx', 'head'), may hold values from -200 to 200
- cache_values: bfloat16 [16384, 1024], P('ctx', 'head'), may hold values from -6 to 6
- cache_lengths: int32 [16], replicated, may hold values from 2 to 1024, as said below
- start_position: int32 [1], replicated, may hold values from 1 to 16384
Outputs:
- attended: bfloat16 [2048, 8192], P('ctx', 'head')
The draws below stay inside these ranges and needn't reach their ends.
Inputs may be any that keep to these rules, and one draw needn't show every extreme that they name: `cache_lengths`: entry c counts the live rows of cache shard c from its first row; some shard is full.
All inputs are finite; a program needn't handle non-finite values.
Results may differ from the reference program's by a relative error of at most 0.015.
The reference program's roundings to bfloat16 on the way count: a program that leaves them out, or rounds other values in their place, can miss the bound.
Values may be sent and summed in bfloat16 or wider, within the bound.
No kernel may reach another device: no remote copies, remote signals or barrier semaphores. Data moves between devices by JAX's collectives and lax.ppermute only.
A program may use at most 192 MiB of HBM per device.

```python
import jax
import jax.numpy as jnp
from jax import lax

D = 8192
HEADS = 64
KV_HEADS = 8
HEAD_DIM = 128
TOK_DEV = 128
CACHE_DEV = 1024
SHARDS = 16
TOKENS = 2048
CACHE = 16384


def draw_cache_lengths(key, part):
    drawn = jax.random.randint(key, (SHARDS,), 2, CACHE_DEV + 1, dtype=jnp.int32)
    chosen = jax.random.randint(jax.random.fold_in(key, 5), (), 0, SHARDS, dtype=jnp.int32)
    return jnp.where(jnp.arange(SHARDS, dtype=jnp.int32) == chosen, CACHE_DEV, drawn).astype(jnp.int32)


def draw_cache_keys(key, part):
    width = KV_HEADS * HEAD_DIM
    return jnp.clip(jax.random.normal(key, (CACHE, width), jnp.float32), -6.0, 6.0).astype(jnp.bfloat16)


def block_scale(rng, dims, pieces, least, largest):
    def one(dim, blocks):
        steps = jax.random.uniform(jax.random.fold_in(jax.random.fold_in(rng, 6), dim), (blocks,), jnp.float32, least / len(pieces), largest / len(pieces))
        return jnp.repeat(jnp.exp(steps), dims[dim] // blocks).reshape((-1,) + (1,) * (len(dims) - dim - 1))

    factor_of = one(*pieces[0])
    for cut in pieces[1:]:
        factor_of = factor_of * one(*cut)
    return factor_of


def scatter_about(key, extent, scale, most, pieces=(), kind=jnp.bfloat16):
    loudness = block_scale(key, extent, pieces, -0.22, 0.18) if pieces else 1.0
    array = jax.random.normal(key, extent, jnp.float32) * scale * loudness
    return jnp.minimum(jnp.maximum(array, -most), most).astype(kind)


def setup_inputs(seed: int = 0) -> dict:
    keys = jax.random.split(jax.random.key(seed), 10)
    tokens = scatter_about(keys[0], (TOKENS, D), 1.0, 6.0, ((0, 16), (1, 8)))
    norm_gain = jnp.clip(1.0 + 0.18 * jax.random.normal(keys[1], (D,), jnp.float32), 0.1, 1.9)
    query_weight = scatter_about(keys[2], (D, HEADS * HEAD_DIM), D ** -0.5, 0.0625, ((1, 8),))
    key_weight = scatter_about(keys[3], (D, KV_HEADS * HEAD_DIM), D ** -0.5, 0.0625, ((1, 8),))
    value_weight = scatter_about(keys[4], (D, KV_HEADS * HEAD_DIM), D ** -0.5, 0.0625, ((1, 8),))
    cache_keys = draw_cache_keys(jax.random.fold_in(keys[9], 71), 0)
    cache_values = scatter_about(keys[6], (CACHE, KV_HEADS * HEAD_DIM), 1.0, 6.0, ((0, 16), (1, 8)))
    cache_lengths = draw_cache_lengths(jax.random.fold_in(keys[9], 71), 0)
    start_position = jax.random.randint(keys[8], (1,), 1, CACHE + 1).astype(jnp.int32)
    return dict(tokens=tokens, norm_gain=norm_gain, query_weight=query_weight, key_weight=key_weight, value_weight=value_weight, cache_keys=cache_keys, cache_values=cache_values, cache_lengths=cache_lengths, start_position=start_position)


epsilon = 1e-05
rope_base = 500000.0
masked_score = -1e+30

def rotary(inputs, position):
    half = inputs.shape[-1] // 2
    freqs = jnp.power(jnp.float32(rope_base), -2.0 * jnp.arange(half, dtype=jnp.float32) / inputs.shape[-1])
    angles = position[:, None] * freqs[None, :]
    cosine = jnp.cos(angles)[:, None, :]
    sine = jnp.sin(angles)[:, None, :]
    first_half = inputs[..., :half]
    second_half = inputs[..., half:]
    return jnp.concatenate([first_half * cosine - second_half * sine, second_half * cosine + first_half * sine], -1)

def reference(tokens, norm_gain, query_weight, key_weight, value_weight, cache_keys, cache_values, cache_lengths, start_position):
    floats = tokens.astype(jnp.float32)
    inverse = lax.rsqrt(lax.optimization_barrier(jnp.mean(floats * floats, -1, keepdims=True)) + epsilon)
    normed = (floats * inverse * norm_gain).astype(jnp.bfloat16)
    position = (start_position[0] + jnp.arange(TOKENS, dtype=jnp.int32)).astype(jnp.float32)
    projected = jnp.dot(normed, query_weight, preferred_element_type=jnp.float32)
    queries = rotary(projected.reshape(TOKENS, HEADS, HEAD_DIM), position).astype(jnp.bfloat16)
    key_proj = jnp.dot(normed, key_weight, preferred_element_type=jnp.float32)
    fresh_keys = rotary(key_proj.reshape(TOKENS, KV_HEADS, HEAD_DIM), position).astype(jnp.bfloat16)
    fresh_values = jnp.dot(normed, value_weight, preferred_element_type=jnp.float32).astype(jnp.bfloat16)
    fresh_values = fresh_values.reshape(TOKENS, KV_HEADS, HEAD_DIM)
    cache_live = jnp.arange(CACHE_DEV, dtype=jnp.int32)[None, :] < cache_lengths[:, None]
    group = HEADS // KV_HEADS
    cache_key_heads = cache_keys.reshape(SHARDS, CACHE_DEV, KV_HEADS, HEAD_DIM).transpose(2, 0, 1, 3)
    cache_value_heads = cache_values.reshape(SHARDS, CACHE_DEV, KV_HEADS, HEAD_DIM).transpose(2, 0, 1, 3)
    fresh_key_heads = fresh_keys.transpose(1, 0, 2)
    fresh_value_heads = fresh_values.transpose(1, 0, 2)
    grouped = queries.reshape(SHARDS, TOK_DEV, KV_HEADS, group, HEAD_DIM).transpose(2, 0, 1, 3, 4)

    def per_head(inputs):
        head_queries, ckeys, cvalues, fkeys, fvalues = inputs
        ckey_float = ckeys.astype(jnp.float32)
        cvalue_float = cvalues.astype(jnp.float32)
        fkey_float = fkeys.astype(jnp.float32)
        fvalue_float = fvalues.astype(jnp.float32)

        def per_block(block_inputs):
            block_queries, block_index = block_inputs
            query_float = block_queries.astype(jnp.float32)
            scale = HEAD_DIM ** (-0.5)
            cscores = jnp.einsum('tgd,skd->tgsk', query_float, ckey_float) * scale
            clive = cache_live[None, None, :, :]
            cscores = jnp.where(clive, cscores, masked_score)
            chigh = lax.optimization_barrier(jnp.max(cscores, -1))
            cweights = jnp.where(clive, jnp.exp(cscores - chigh[..., None]), 0.0)
            ctotal = lax.optimization_barrier(jnp.sum(cweights, -1))
            crounded = lax.optimization_barrier(cweights.astype(jnp.bfloat16)).astype(jnp.float32)
            cmixed = jnp.einsum('tgsk,skd->tgsd', crounded, cvalue_float)
            cpart = lax.optimization_barrier((cmixed / ctotal[..., None]).astype(jnp.bfloat16)).astype(jnp.float32)
            clse = chigh + jnp.log(ctotal)
            fscores = jnp.einsum('tgd,kd->tgk', query_float, fkey_float) * scale
            query_pos = block_index * TOK_DEV + jnp.arange(TOK_DEV, dtype=jnp.int32)
            flive = (jnp.arange(TOKENS, dtype=jnp.int32)[None, :] <= query_pos[:, None])[:, None, :]
            fscores = jnp.where(flive, fscores, masked_score)
            fhigh = lax.optimization_barrier(jnp.max(fscores, -1))
            fweights = jnp.where(flive, jnp.exp(fscores - fhigh[..., None]), 0.0)
            ftotal = lax.optimization_barrier(jnp.sum(fweights, -1))
            frounded = lax.optimization_barrier(fweights.astype(jnp.bfloat16)).astype(jnp.float32)
            fmixed = jnp.einsum('tgk,kd->tgd', frounded, fvalue_float)
            top = jnp.maximum(lax.optimization_barrier(jnp.max(clse, -1)), fhigh)
            cscale = jnp.exp(clse - top[..., None])
            fscale = jnp.exp(fhigh - top)
            numer = lax.optimization_barrier(jnp.sum(cpart * cscale[..., None], 2)) + fmixed * fscale[..., None]
            denom = lax.optimization_barrier(jnp.sum(cscale, -1)) + ftotal * fscale
            return numer / denom[..., None]
        return lax.map(per_block, (head_queries, jnp.arange(SHARDS, dtype=jnp.int32)))
    outputs = lax.map(per_head, (grouped, cache_key_heads, cache_value_heads, fresh_key_heads, fresh_value_heads))
    return outputs.transpose(1, 2, 0, 3, 4).reshape(TOKENS, HEADS * HEAD_DIM).astype(jnp.bfloat16)
```

```python
import functools

import jax
import jax.numpy as jnp
from jax import lax
from jax.experimental import pallas as pl
from jax.experimental.pallas import tpu as pltpu
from jax.sharding import PartitionSpec as P

HEAD_DIM = 128
EPSILON = 1e-05
ROPE_BASE = 500000.0
MASKED = -1e30
KEY_BLOCK = 256
ROW_BLOCK = 256
EXP2_SCALE = HEAD_DIM**-0.5 * 1.4426950408889634


X_CHIPS = 4
Z_CHIPS = 4
OFFSETS = ((0, 0), (1, 0), (0, -1), (0, 1), (1, -1), (1, 1), (0, 2), (1, 2))


def shift_ctx(x, dy, dx, dc):
    pairs = []
    for y in range(2):
        for c in range(X_CHIPS):
            for core in range(2):
                source = (y * X_CHIPS + c) * 2 + core
                target = (((y + dy) % 2) * X_CHIPS + (c + dx) % X_CHIPS) * 2 + (core + dc) % 2
                pairs.append((source, target))
    return lax.ppermute(x, "ctx", pairs)


def shift_head(x, dy, dz):
    pairs = []
    for y in range(2):
        for z in range(Z_CHIPS):
            pairs.append((y * Z_CHIPS + z, ((y + dy) % 2) * Z_CHIPS + (z + dz) % Z_CHIPS))
    return lax.ppermute(x, "head", pairs)


def ring_gather(x, shift):
    partner = shift(x, 1, 0)
    right = shift(x, 0, 1)
    left = shift(x, 0, -1)
    partner_right = shift(partner, 0, 1)
    partner_left = shift(partner, 0, -1)
    far = shift(right, 0, 1)
    partner_far = shift(partner_left, 0, -1)
    return [x, partner, right, left, partner_right, partner_left, far, partner_far]


def project_kernel(order_ref, *refs):
    pieces = refs[:8]
    gain_ref, cos_ref, sin_ref, wq_ref, wk_ref, wv_ref = refs[8:14]
    q_ref, kv_ref = refs[14:16]
    tok, wq, wk, wv, accq, acck, accv, tok_sem, w_sem = refs[16:]
    depth = tok.shape[2]
    copies = []
    for j in range(8):
        copies.append(pltpu.make_async_copy(pieces[j], tok.at[j], tok_sem.at[j]))
    for c in copies:
        c.start()

    def weight_copies(j):
        rows = pl.ds(pl.multiple_of(order_ref[j] * depth, depth), depth)
        return (
            pltpu.make_async_copy(wk_ref.at[rows], wk.at[j], w_sem.at[j, 0]),
            pltpu.make_async_copy(wv_ref.at[rows], wv.at[j], w_sem.at[j, 1]),
            pltpu.make_async_copy(wq_ref.at[rows], wq.at[j], w_sem.at[j, 2]),
        )

    for j in range(8):
        for c in weight_copies(j):
            c.start()
    total = jnp.zeros((tok.shape[1], 1), jnp.float32)
    for j in range(8):
        copies[j].wait()
        floats = tok[j].astype(jnp.float32)
        total = total + jnp.sum(floats * floats, axis=1, keepdims=True)
    inverse = lax.rsqrt(total / (8 * depth) + EPSILON)
    accq[...] = jnp.zeros_like(accq)
    acck[...] = jnp.zeros_like(acck)
    accv[...] = jnp.zeros_like(accv)

    def step(j, carry):
        gain = gain_ref[pl.ds(order_ref[j], 1), :]
        normed = (tok[j].astype(jnp.float32) * inverse * gain).astype(jnp.bfloat16)
        for c in weight_copies(j):
            c.wait()
        acck[...] += jnp.dot(normed, wk[j], preferred_element_type=jnp.float32)
        accv[...] += jnp.dot(normed, wv[j], preferred_element_type=jnp.float32)
        accq[...] += jnp.dot(normed, wq[j], preferred_element_type=jnp.float32)
        return carry

    lax.fori_loop(0, 8, step, 0)
    cosine, sine = cos_ref[...], sin_ref[...]

    def rotary(u):
        return (u * cosine + pltpu.roll(u, HEAD_DIM // 2, 1) * sine).astype(jnp.bfloat16)

    for g in range(accq.shape[1] // HEAD_DIM):
        q_ref[g] = rotary(accq[:, g * HEAD_DIM : (g + 1) * HEAD_DIM])
    new_key = rotary(acck[...])
    new_value = accv[...].astype(jnp.bfloat16)
    for c in range(kv_ref.shape[0]):
        kv_ref[c, 0] = new_key
        kv_ref[c, 1] = new_value


def project(order, pieces, gain, cosine, sine, wq, wk, wv, shards):
    rows, depth = pieces[0].shape
    q_width, kv_width = wq.shape[1], wk.shape[1]
    any_spec = pl.BlockSpec(memory_space=pl.ANY)
    vmem_spec = pl.BlockSpec(memory_space=pltpu.VMEM)
    return pl.pallas_call(
        project_kernel,
        out_shape=(
            jax.ShapeDtypeStruct((q_width // HEAD_DIM, rows, HEAD_DIM), jnp.bfloat16),
            jax.ShapeDtypeStruct((shards, 2, rows, kv_width), jnp.bfloat16),
        ),
        in_specs=[pl.BlockSpec(memory_space=pltpu.SMEM)]
        + [any_spec] * 8
        + [vmem_spec] * 3
        + [any_spec] * 3,
        out_specs=(vmem_spec, vmem_spec),
        scratch_shapes=[
            pltpu.VMEM((8, rows, depth), jnp.bfloat16),
            pltpu.VMEM((8, depth, q_width), jnp.bfloat16),
            pltpu.VMEM((8, depth, kv_width), jnp.bfloat16),
            pltpu.VMEM((8, depth, kv_width), jnp.bfloat16),
            pltpu.VMEM((rows, q_width), jnp.float32),
            pltpu.VMEM((rows, kv_width), jnp.float32),
            pltpu.VMEM((rows, kv_width), jnp.float32),
            pltpu.SemaphoreType.DMA((8,)),
            pltpu.SemaphoreType.DMA((8, 3)),
        ],
        compiler_params=pltpu.CompilerParams(vmem_limit_bytes=50 * 2**20),
        cost_estimate=pl.CostEstimate(
            flops=2 * rows * 8 * depth * (q_width + 2 * kv_width),
            bytes_accessed=2 * 8 * depth * (q_width + 2 * kv_width + rows),
            transcendentals=0,
        ),
        name="project",
    )(order, *pieces, gain, cosine, sine, wq, wk, wv)


def attend_kernel(count, first, last, *refs):
    refs = list(refs)
    lens_ref, q_ref = refs[:2]
    blocks = refs[2 : 2 + count]
    refs = refs[2 + count :]
    if last:
        fresh_ref = refs.pop(0)
    if not first:
        m_in, l_in, acc_in = refs[:3]
        refs = refs[3:]
    if last:
        out_ref = refs.pop(0)
        kv, fresh, sem, fresh_sem, m_ref, l_ref, acc_ref = refs
    else:
        m_ref, l_ref, acc_ref = refs[:3]
        kv, sem = refs[3:]
    for j in range(count):
        pltpu.make_async_copy(blocks[j], kv.at[j], sem.at[j]).start()
    if last:
        fresh_copies = []
        tokens_each = fresh_ref.shape[2]
        for f in range(fresh_ref.shape[0]):
            for i in range(2):
                fresh_copies.append(
                    pltpu.make_async_copy(
                        fresh_ref.at[f, i],
                        fresh.at[i, pl.ds(f * tokens_each, tokens_each)],
                        fresh_sem.at[f, i],
                    )
                )
        for c in fresh_copies:
            c.start()
    if first:
        m_ref[...] = jnp.full_like(m_ref, MASKED)
        l_ref[...] = jnp.zeros_like(l_ref)
        acc_ref[...] = jnp.zeros_like(acc_ref)
    else:
        m_ref[...] = m_in[...]
        l_ref[...] = l_in[...]
        acc_ref[...] = acc_in[...]
    heads, rows, _ = q_ref.shape
    per = ROW_BLOCK // rows

    def block(keys, values, live_of):
        for r in range(heads // per):
            at = pl.ds(r * ROW_BLOCK, ROW_BLOCK)
            q = q_ref[r * per : (r + 1) * per].reshape(ROW_BLOCK, HEAD_DIM)
            s = lax.dot_general(
                q, keys, (((1,), (1,)), ((), ())), preferred_element_type=jnp.float32
            )
            s = jnp.where(live_of, s, MASKED)
            m_old = m_ref[at, :]
            m_new = jnp.maximum(m_old, jnp.max(s, axis=1, keepdims=True))
            alpha = jnp.exp2((m_old - m_new) * EXP2_SCALE)
            parts = []
            total = l_ref[at, :] * alpha
            for c in range(KEY_BLOCK // 128):
                p = jnp.exp2((s[:, c * 128 : (c + 1) * 128] - m_new) * EXP2_SCALE)
                total = total + p
                parts.append(p.astype(jnp.bfloat16))
            m_ref[at, :] = m_new
            l_ref[at, :] = total
            acc_ref[at, :] = acc_ref[at, :] * alpha + jnp.dot(
                jnp.concatenate(parts, axis=1), values, preferred_element_type=jnp.float32
            )

    column = lax.broadcasted_iota(jnp.int32, (ROW_BLOCK, KEY_BLOCK), 1)

    def shard(j, carry):
        pltpu.make_async_copy(blocks[0], kv.at[j], sem.at[j]).wait()
        length = lens_ref[j]

        def one(b, c):
            at = pl.ds(pl.multiple_of(b * KEY_BLOCK, KEY_BLOCK), KEY_BLOCK)
            block(kv[j, 0, at, :], kv[j, 1, at, :], column < length - b * KEY_BLOCK)
            return c

        return lax.fori_loop(0, (length + KEY_BLOCK - 1) // KEY_BLOCK, one, carry)

    if count:
        lax.fori_loop(0, count, shard, 0)
    if last:
        for c in fresh_copies:
            c.wait()
        start = lens_ref[16] * rows
        row = lax.broadcasted_iota(jnp.int32, (ROW_BLOCK, KEY_BLOCK), 0) % rows

        def one_fresh(b, c):
            at = pl.ds(pl.multiple_of(b * KEY_BLOCK, KEY_BLOCK), KEY_BLOCK)
            block(fresh[0, at, :], fresh[1, at, :], column <= row + (start - b * KEY_BLOCK))
            return c

        lax.fori_loop(0, (start + rows + KEY_BLOCK - 1) // KEY_BLOCK, one_fresh, 0)
        for g in range(heads):
            at = pl.ds(g * rows, rows)
            total = jnp.sum(l_ref[at, :], axis=1, keepdims=True)
            out_ref[:, g * HEAD_DIM : (g + 1) * HEAD_DIM] = (acc_ref[at, :] / total).astype(
                out_ref.dtype
            )


def attend(lens, q, blocks, fresh, state, expect):
    heads, rows, _ = q.shape
    count = len(blocks)
    first, last = state is None, fresh is not None
    any_spec = pl.BlockSpec(memory_space=pl.ANY)
    vmem_spec = pl.BlockSpec(memory_space=pltpu.VMEM)
    wide = (heads * rows, HEAD_DIM)
    in_specs = [pl.BlockSpec(memory_space=pltpu.SMEM), vmem_spec] + [any_spec] * count
    args = [lens, q, *blocks]
    scratch = []
    if count:
        scratch.append(pltpu.VMEM((count, *blocks[0].shape), jnp.bfloat16))
    if last:
        args.append(fresh)
        in_specs.append(any_spec)
        shards, _, each, width = fresh.shape
        scratch.append(pltpu.VMEM((2, shards * each, width), jnp.bfloat16))
    if count:
        scratch.append(pltpu.SemaphoreType.DMA((count,)))
    if not first:
        args += state
        in_specs += [vmem_spec] * 3
    if last:
        scratch += [pltpu.SemaphoreType.DMA((shards, 2))]
        scratch += [pltpu.VMEM(wide, jnp.float32)] * 3
        out_shape = jax.ShapeDtypeStruct((rows, heads * HEAD_DIM), jnp.bfloat16)
        out_specs = vmem_spec
    else:
        out_shape = (jax.ShapeDtypeStruct(wide, jnp.float32),) * 3
        out_specs = (vmem_spec,) * 3
    return pl.pallas_call(
        functools.partial(attend_kernel, count, first, last),
        out_shape=out_shape,
        in_specs=in_specs,
        out_specs=out_specs,
        scratch_shapes=scratch,
        compiler_params=pltpu.CompilerParams(vmem_limit_bytes=50 * 2**20),
        cost_estimate=pl.CostEstimate(
            flops=4 * heads * rows * HEAD_DIM * expect,
            bytes_accessed=2**19 * count,
            transcendentals=heads * rows * expect,
        ),
        name="attend",
    )(*args)


def body(
    tokens,
    norm_gain,
    query_weight,
    key_weight,
    value_weight,
    cache_keys,
    cache_values,
    cache_lengths,
    start_position,
):
    shards = lax.axis_size("ctx")
    rank = lax.axis_index("ctx")
    place = lax.axis_index("head")
    rows, depth = tokens.shape
    pieces = ring_gather(tokens, shift_head)
    y_lo, z = place // Z_CHIPS, place % Z_CHIPS
    order = jnp.stack(
        [(y_lo + dy) % 2 * Z_CHIPS + (z + dz) % Z_CHIPS for dy, dz in OFFSETS]
    ).astype(jnp.int32)

    kv = jnp.stack([cache_keys, cache_values])
    mine = ring_gather(kv, lambda x, dy, dx: shift_ctx(x, dy, dx, 0))
    theirs = [shift_ctx(x, 0, 0, 1) for x in mine]
    y_hi, x, core = rank // (2 * X_CHIPS), rank // 2 % X_CHIPS, rank % 2
    owners = [
        (((y_hi + dy) % 2) * X_CHIPS + (x + dx) % X_CHIPS) * 2 + (core + dc) % 2
        for dc in range(2)
        for dy, dx in OFFSETS
    ]
    lens = jnp.concatenate(
        [jnp.take(cache_lengths, jnp.stack(owners)), jnp.reshape(rank, (1,))]
    ).astype(jnp.int32)

    position = (start_position[0] + rank * rows + jnp.arange(rows, dtype=jnp.int32)).astype(
        jnp.float32
    )
    half = HEAD_DIM // 2
    freqs = jnp.power(
        jnp.float32(ROPE_BASE), -2.0 * jnp.arange(half, dtype=jnp.float32) / HEAD_DIM
    )
    angles = position[:, None] * freqs[None, :]
    cosine, sine = jnp.cos(angles), jnp.sin(angles)
    cosine = jnp.concatenate([cosine, cosine], 1)
    sine = jnp.concatenate([-sine, sine], 1)

    q, fresh_out = project(
        order,
        pieces,
        norm_gain.reshape(8, depth),
        cosine,
        sine,
        query_weight,
        key_weight,
        value_weight,
        shards,
    )
    fresh = lax.all_to_all(fresh_out, "ctx", split_axis=0, concat_axis=0, tiled=True)
    return attend(lens, q, mine + theirs, fresh, None, 9000)


def solution(mesh):
    in_specs = (
        P("ctx", "head"),
        P(),
        P(None, "head"),
        P(None, "head"),
        P(None, "head"),
        P("ctx", "head"),
        P("ctx", "head"),
        P(),
        P(),
    )
    out_specs = P("ctx", "head")
    return jax.shard_map(body, mesh=mesh, in_specs=in_specs, out_specs=out_specs, check_vma=False)
```

```python
import functools

import jax
import jax.numpy as jnp
from jax import lax
from jax.experimental import pallas as pl
from jax.experimental.pallas import tpu as pltpu
from jax.sharding import PartitionSpec as P

HEAD_DIM = 128
EPSILON = 1e-05
ROPE_BASE = 500000.0
MASKED = -1e30
KEY_BLOCK = 256
ROW_BLOCK = 512
EXP2_SCALE = HEAD_DIM**-0.5 * 1.4426950408889634


X_CHIPS = 4
Z_CHIPS = 4
OFFSETS = ((0, 0), (1, 0), (0, -1), (0, 1), (1, -1), (1, 1), (0, 2), (1, 2))


def shift_ctx(x, dy, dx, dc):
    pairs = []
    for y in range(2):
        for c in range(X_CHIPS):
            for core in range(2):
                source = (y * X_CHIPS + c) * 2 + core
                target = (((y + dy) % 2) * X_CHIPS + (c + dx) % X_CHIPS) * 2 + (core + dc) % 2
                pairs.append((source, target))
    return lax.ppermute(x, "ctx", pairs)


def shift_head(x, dy, dz):
    pairs = []
    for y in range(2):
        for z in range(Z_CHIPS):
            pairs.append((y * Z_CHIPS + z, ((y + dy) % 2) * Z_CHIPS + (z + dz) % Z_CHIPS))
    return lax.ppermute(x, "head", pairs)


def ring_gather(x, shift, after=None):
    partner = shift(x if after is None else lax.optimization_barrier((x, *after))[0], 1, 0)
    right = shift(x, 0, 1)
    left = shift(x, 0, -1)
    partner_right = shift(partner, 0, 1)
    partner_left = shift(partner, 0, -1)
    far = shift(right, 0, 1)
    partner_far = shift(partner_left, 0, -1)
    return [x, partner, right, left, partner_right, partner_left, far, partner_far]


def project_kernel(order_ref, *refs):
    pieces = refs[:8]
    gain_ref, cos_ref, sin_ref, wq_ref, wk_ref, wv_ref = refs[8:14]
    q_ref, kv_ref = refs[14:16]
    tok, wq, wk, wv, accq, acck, accv, tok_sem, w_sem = refs[16:]
    depth = tok.shape[2]
    copies = []
    for j in range(8):
        copies.append(pltpu.make_async_copy(pieces[j], tok.at[j], tok_sem.at[j]))
    for c in copies:
        c.start()

    def weight_copies(j):
        rows = pl.ds(pl.multiple_of(order_ref[j] * depth, depth), depth)
        return (
            pltpu.make_async_copy(wk_ref.at[rows], wk.at[j], w_sem.at[j, 0]),
            pltpu.make_async_copy(wv_ref.at[rows], wv.at[j], w_sem.at[j, 1]),
            pltpu.make_async_copy(wq_ref.at[rows], wq.at[j], w_sem.at[j, 2]),
        )

    for j in range(8):
        for c in weight_copies(j):
            c.start()
    total = jnp.zeros((tok.shape[1], 1), jnp.float32)
    for j in range(8):
        copies[j].wait()
        floats = tok[j].astype(jnp.float32)
        total = total + jnp.sum(floats * floats, axis=1, keepdims=True)
    inverse = lax.rsqrt(total / (8 * depth) + EPSILON)
    accq[...] = jnp.zeros_like(accq)
    acck[...] = jnp.zeros_like(acck)
    accv[...] = jnp.zeros_like(accv)

    def step(j, carry):
        gain = gain_ref[pl.ds(order_ref[j], 1), :]
        normed = (tok[j].astype(jnp.float32) * inverse * gain).astype(jnp.bfloat16)
        for c in weight_copies(j):
            c.wait()
        acck[...] += jnp.dot(normed, wk[j], preferred_element_type=jnp.float32)
        accv[...] += jnp.dot(normed, wv[j], preferred_element_type=jnp.float32)
        accq[...] += jnp.dot(normed, wq[j], preferred_element_type=jnp.float32)
        return carry

    lax.fori_loop(0, 8, step, 0)
    cosine, sine = cos_ref[...], sin_ref[...]

    def rotary(u):
        return (u * cosine + pltpu.roll(u, HEAD_DIM // 2, 1) * sine).astype(jnp.bfloat16)

    for g in range(accq.shape[1] // HEAD_DIM):
        q_ref[g] = rotary(accq[:, g * HEAD_DIM : (g + 1) * HEAD_DIM])
    new_key = rotary(acck[...])
    new_value = accv[...].astype(jnp.bfloat16)
    for c in range(kv_ref.shape[0]):
        kv_ref[c, 0] = new_key
        kv_ref[c, 1] = new_value


def project(order, pieces, gain, cosine, sine, wq, wk, wv, shards):
    rows, depth = pieces[0].shape
    q_width, kv_width = wq.shape[1], wk.shape[1]
    any_spec = pl.BlockSpec(memory_space=pl.ANY)
    vmem_spec = pl.BlockSpec(memory_space=pltpu.VMEM)
    return pl.pallas_call(
        project_kernel,
        out_shape=(
            jax.ShapeDtypeStruct((q_width // HEAD_DIM, rows, HEAD_DIM), jnp.bfloat16),
            jax.ShapeDtypeStruct((shards, 2, rows, kv_width), jnp.bfloat16),
        ),
        in_specs=[pl.BlockSpec(memory_space=pltpu.SMEM)]
        + [any_spec] * 8
        + [vmem_spec] * 3
        + [any_spec] * 3,
        out_specs=(vmem_spec, vmem_spec),
        scratch_shapes=[
            pltpu.VMEM((8, rows, depth), jnp.bfloat16),
            pltpu.VMEM((8, depth, q_width), jnp.bfloat16),
            pltpu.VMEM((8, depth, kv_width), jnp.bfloat16),
            pltpu.VMEM((8, depth, kv_width), jnp.bfloat16),
            pltpu.VMEM((rows, q_width), jnp.float32),
            pltpu.VMEM((rows, kv_width), jnp.float32),
            pltpu.VMEM((rows, kv_width), jnp.float32),
            pltpu.SemaphoreType.DMA((8,)),
            pltpu.SemaphoreType.DMA((8, 3)),
        ],
        compiler_params=pltpu.CompilerParams(vmem_limit_bytes=50 * 2**20),
        cost_estimate=pl.CostEstimate(
            flops=2 * rows * 8 * depth * (q_width + 2 * kv_width),
            bytes_accessed=2 * 8 * depth * (q_width + 2 * kv_width + rows),
            transcendentals=0,
        ),
        name="project",
    )(order, *pieces, gain, cosine, sine, wq, wk, wv)


def attend_kernel(base, count, first, last, *refs):
    refs = list(refs)
    lens_ref, q_ref = refs[:2]
    blocks = refs[2 : 2 + count]
    refs = refs[2 + count :]
    if last:
        fresh_ref = refs.pop(0)
    if not first:
        m_in, l_in, acc_in = refs[:3]
        refs = refs[3:]
    if last:
        out_ref = refs.pop(0)
        kv, fresh, sem, fresh_sem, m_ref, l_ref, acc_ref = refs
    else:
        m_ref, l_ref, acc_ref = refs[:3]
        kv, sem = refs[3:]
    for j in range(count):
        pltpu.make_async_copy(blocks[j], kv.at[j], sem.at[j]).start()
    if last:
        fresh_copies = []
        tokens_each = fresh_ref.shape[2]
        for f in range(fresh_ref.shape[0]):
            for i in range(2):
                fresh_copies.append(
                    pltpu.make_async_copy(
                        fresh_ref.at[f, i],
                        fresh.at[i, pl.ds(f * tokens_each, tokens_each)],
                        fresh_sem.at[f, i],
                    )
                )
        for c in fresh_copies:
            c.start()
    if first:
        m_ref[...] = jnp.full_like(m_ref, MASKED)
        l_ref[...] = jnp.zeros_like(l_ref)
        acc_ref[...] = jnp.zeros_like(acc_ref)
    else:
        m_ref[...] = m_in[...]
        l_ref[...] = l_in[...]
        acc_ref[...] = acc_in[...]
    heads, rows, _ = q_ref.shape
    per = ROW_BLOCK // rows

    def block(keys, values, live_of):
        for r in range(heads // per):
            at = pl.ds(r * ROW_BLOCK, ROW_BLOCK)
            q = q_ref[r * per : (r + 1) * per].reshape(ROW_BLOCK, HEAD_DIM)
            s = lax.dot_general(
                q, keys, (((1,), (1,)), ((), ())), preferred_element_type=jnp.float32
            )
            s = jnp.where(live_of, s, MASKED)
            m_old = m_ref[at, :]
            m_new = jnp.maximum(m_old, jnp.max(s, axis=1, keepdims=True))
            alpha = jnp.exp2((m_old - m_new) * EXP2_SCALE)
            parts = []
            total = l_ref[at, :] * alpha
            for c in range(KEY_BLOCK // 128):
                p = jnp.exp2((s[:, c * 128 : (c + 1) * 128] - m_new) * EXP2_SCALE)
                total = total + p
                parts.append(p.astype(jnp.bfloat16))
            m_ref[at, :] = m_new
            l_ref[at, :] = total
            acc_ref[at, :] = acc_ref[at, :] * alpha + jnp.dot(
                jnp.concatenate(parts, axis=1), values, preferred_element_type=jnp.float32
            )

    column = lax.broadcasted_iota(jnp.int32, (ROW_BLOCK, KEY_BLOCK), 1)

    def shard(j, carry):
        pltpu.make_async_copy(blocks[0], kv.at[j], sem.at[j]).wait()
        length = lens_ref[base + j]

        def one(b, c):
            at = pl.ds(pl.multiple_of(b * KEY_BLOCK, KEY_BLOCK), KEY_BLOCK)
            block(kv[j, 0, at, :], kv[j, 1, at, :], column < length - b * KEY_BLOCK)
            return c

        return lax.fori_loop(0, (length + KEY_BLOCK - 1) // KEY_BLOCK, one, carry)

    if count:
        lax.fori_loop(0, count, shard, 0)
    if last:
        for c in fresh_copies:
            c.wait()
        start = lens_ref[16] * rows
        row = lax.broadcasted_iota(jnp.int32, (ROW_BLOCK, KEY_BLOCK), 0) % rows

        def one_fresh(b, c):
            at = pl.ds(pl.multiple_of(b * KEY_BLOCK, KEY_BLOCK), KEY_BLOCK)
            block(fresh[0, at, :], fresh[1, at, :], column <= row + (start - b * KEY_BLOCK))
            return c

        lax.fori_loop(0, (start + rows + KEY_BLOCK - 1) // KEY_BLOCK, one_fresh, 0)
        for g in range(heads):
            at = pl.ds(g * rows, rows)
            total = jnp.sum(l_ref[at, :], axis=1, keepdims=True)
            out_ref[:, g * HEAD_DIM : (g + 1) * HEAD_DIM] = (acc_ref[at, :] / total).astype(
                out_ref.dtype
            )


def attend(lens, base, q, blocks, fresh, state, expect):
    heads, rows, _ = q.shape
    count = len(blocks)
    first, last = state is None, fresh is not None
    any_spec = pl.BlockSpec(memory_space=pl.ANY)
    vmem_spec = pl.BlockSpec(memory_space=pltpu.VMEM)
    wide = (heads * rows, HEAD_DIM)
    in_specs = [pl.BlockSpec(memory_space=pltpu.SMEM), vmem_spec] + [any_spec] * count
    args = [lens, q, *blocks]
    scratch = []
    if count:
        scratch.append(pltpu.VMEM((count, *blocks[0].shape), jnp.bfloat16))
    if last:
        args.append(fresh)
        in_specs.append(any_spec)
        shards, _, each, width = fresh.shape
        scratch.append(pltpu.VMEM((2, shards * each, width), jnp.bfloat16))
    if count:
        scratch.append(pltpu.SemaphoreType.DMA((count,)))
    if not first:
        args += state
        in_specs += [vmem_spec] * 3
    if last:
        scratch += [pltpu.SemaphoreType.DMA((shards, 2))]
        scratch += [pltpu.VMEM(wide, jnp.float32)] * 3
        out_shape = jax.ShapeDtypeStruct((rows, heads * HEAD_DIM), jnp.bfloat16)
        out_specs = vmem_spec
    else:
        out_shape = (jax.ShapeDtypeStruct(wide, jnp.float32),) * 3
        out_specs = (vmem_spec,) * 3
    return pl.pallas_call(
        functools.partial(attend_kernel, base, count, first, last),
        out_shape=out_shape,
        in_specs=in_specs,
        out_specs=out_specs,
        scratch_shapes=scratch,
        compiler_params=pltpu.CompilerParams(vmem_limit_bytes=50 * 2**20),
        cost_estimate=pl.CostEstimate(
            flops=4 * heads * rows * HEAD_DIM * expect,
            bytes_accessed=2**19 * count,
            transcendentals=heads * rows * expect,
        ),
        name="attend",
    )(*args)


def body(
    tokens,
    norm_gain,
    query_weight,
    key_weight,
    value_weight,
    cache_keys,
    cache_values,
    cache_lengths,
    start_position,
):
    shards = lax.axis_size("ctx")
    rank = lax.axis_index("ctx")
    place = lax.axis_index("head")
    rows, depth = tokens.shape
    pieces = ring_gather(tokens, shift_head)
    y_lo, z = place // Z_CHIPS, place % Z_CHIPS
    order = jnp.stack(
        [(y_lo + dy) % 2 * Z_CHIPS + (z + dz) % Z_CHIPS for dy, dz in OFFSETS]
    ).astype(jnp.int32)

    kv = jnp.stack([cache_keys, cache_values])
    mine = ring_gather(kv, lambda x, dy, dx: shift_ctx(x, dy, dx, 0), pieces[1:4])
    theirs = [shift_ctx(x, 0, 0, 1) for x in mine]
    y_hi, x, core = rank // (2 * X_CHIPS), rank // 2 % X_CHIPS, rank % 2
    early, late = (0, 2, 3, 1), (4, 5, 6, 7)
    blocks, owners = [], []
    for group in (early, late):
        for dc, arrays in ((0, mine), (1, theirs)):
            for i in group:
                dy, dx = OFFSETS[i]
                blocks.append(arrays[i])
                owners.append(
                    (((y_hi + dy) % 2) * X_CHIPS + (x + dx) % X_CHIPS) * 2 + (core + dc) % 2
                )
    lens = jnp.concatenate(
        [jnp.take(cache_lengths, jnp.stack(owners)), jnp.reshape(rank, (1,))]
    ).astype(jnp.int32)

    position = (start_position[0] + rank * rows + jnp.arange(rows, dtype=jnp.int32)).astype(
        jnp.float32
    )
    half = HEAD_DIM // 2
    freqs = jnp.power(
        jnp.float32(ROPE_BASE), -2.0 * jnp.arange(half, dtype=jnp.float32) / HEAD_DIM
    )
    angles = position[:, None] * freqs[None, :]
    cosine, sine = jnp.cos(angles), jnp.sin(angles)
    cosine = jnp.concatenate([cosine, cosine], 1)
    sine = jnp.concatenate([-sine, sine], 1)

    q, fresh_out = project(
        order,
        pieces,
        norm_gain.reshape(8, depth),
        cosine,
        sine,
        query_weight,
        key_weight,
        value_weight,
        shards,
    )
    fresh = lax.all_to_all(fresh_out, "ctx", split_axis=0, concat_axis=0, tiled=True)
    state = attend(lens, 0, q, blocks[:8], None, None, 4500)
    return attend(lens, 8, q, blocks[8:], fresh, list(state), 4500)


def solution(mesh):
    in_specs = (
        P("ctx", "head"),
        P(),
        P(None, "head"),
        P(None, "head"),
        P(None, "head"),
        P("ctx", "head"),
        P("ctx", "head"),
        P(),
        P(),
    )
    out_specs = P("ctx", "head")
    return jax.shard_map(body, mesh=mesh, in_specs=in_specs, out_specs=out_specs, check_vma=False)
```
